32 devices in a mesh: groups: 2 (over x), gx: 16 (over z, y, core).
Axes of the slice: x: 2, y: 2, z: 4, core: 2. Of those that a mesh axis runs over, the one named last changes fastest.
Arguments:
- tokens: bfloat16 [768, 4608], P('groups', 'gx'), parts along dimension 0, may hold values from -6 to 6
- gate_weight: bfloat16 [16, 576, 9216], P('gx'), may hold values from -0.09375 to 0.09375
- up_weight: bfloat16 [16, 576, 9216], P('gx'), may hold values from -0.09375 to 0.09375
- down_weight: bfloat16 [16, 2304, 2304], P('gx'), may hold values from -0.046875 to 0.046875
Outputs:
- mixed: bfloat16 [768, 4608], P('groups', 'gx'), parts along dimension 0
The draws below stay inside these ranges and needn't reach their ends.
There are 2 independent parts, one for each index of `groups`. The reference program is written for one: setup_inputs(seed, part) draws one part's arguments, and reference() takes and returns one part's arrays. A program takes and returns all parts, laid end to end along the dimension named above; an argument that names none is the same for every part. Nothing has to cross between parts.
All inputs are finite; a program needn't handle non-finite values.
Results may differ from the reference program's by a relative error of at most 0.015.
Values may be sent and summed in bfloat16 or wider, within the bound.
A program may use at most 128 MiB of HBM per device.

```python
import jax
import jax.numpy as jnp

D = 4608
FF = 18432
TOK = 384
XS = 8
YS = 2


def level_of(own_key, shape, cuts, smallest, top_value):
    gain = 1.0
    for position, parts in cuts:
        draws = jax.random.uniform(jax.random.fold_in(jax.random.fold_in(own_key, 6), position), (parts,), jnp.float32, smallest / len(cuts), top_value / len(cuts))
        gain = gain * jnp.repeat(jnp.exp(draws), shape[position] // parts).reshape((-1,) + (1,) * (len(shape) - 1 - position))
    return gain


def scatter_about(rng, shape, spread, reach, cuts=(), kind=jnp.bfloat16):
    result = spread * jax.random.normal(rng, shape, jnp.float32)
    if cuts:
        result = result * level_of(rng, shape, cuts, -0.22, 0.18)
    return jnp.clip(result, -reach, reach).astype(kind)


def setup_inputs(seed: int = 0, part: int = 0) -> dict:
    splits = jax.random.split(jax.random.key(seed), 5)
    part_splits = jax.random.split(jax.random.fold_in(splits[4], part), 5)
    tokens = scatter_about(part_splits[0], (TOK, D), 1.0, 6.0, ((1, 16),))
    gate_weight = scatter_about(splits[1], (XS * YS, D // XS, FF // YS), D ** -0.5, 0.09375, ((0, 16),))
    up_weight = scatter_about(splits[2], (XS * YS, D // XS, FF // YS), D ** -0.5, 0.09375, ((0, 16),))
    down_weight = scatter_about(splits[3], (XS * YS, FF // XS, D // YS), FF ** -0.5, 0.046875, ((0, 16),))
    return {"tokens": tokens, "gate_weight": gate_weight, "up_weight": up_weight, "down_weight": down_weight}


def assemble(tile_stack, row_count, column_count):
    blocks = tile_stack.reshape(YS, XS, YS, -1, tile_stack.shape[2])
    return blocks.transpose(2, 1, 3, 0, 4).reshape(row_count, column_count)


def reference(tokens, gate_weight, up_weight, down_weight):
    gate_full = assemble(gate_weight, D, FF)
    up_full = assemble(up_weight, D, FF)
    down_full = assemble(down_weight, FF, D)
    gate = jnp.dot(tokens, gate_full, preferred_element_type=jnp.float32)
    up_proj = jnp.dot(tokens, up_full, preferred_element_type=jnp.float32)
    hidden = (jax.nn.gelu(gate, approximate=True) * up_proj).astype(jnp.bfloat16)
    mixed = jnp.dot(hidden, down_full, preferred_element_type=jnp.float32)
    return mixed.astype(jnp.bfloat16)
```

```python
import functools

import jax
import jax.numpy as jnp
from jax import lax
from jax.experimental import pallas as pl
from jax.experimental.pallas import tpu as pltpu
from jax.sharding import PartitionSpec as P

XS = 8
PLAN = (2, 4, 3, 2, 1)
Z_ROWS = (1, 3, 2, 1, 1)
VMEM_BYTES = 67043328
MESH = pl.DeviceIdType.MESH
DIAG, ZN, YN, OWN = 0, 1, 2, 3


def from_partner(block, axis, bit):
    count = lax.axis_size(axis)
    route = []
    for low in range(count):
        high = low | 1 << bit
        if high != low and high < count:
            route += [(low, high), (high, low)]
    return lax.ppermute(block, axis, route)


def bit_clear(device_index, bit_number):
    return device_index >> bit_number & 1 == 0


def plain_shards(tokens, gate_weight, up_weight, down_weight):
    gate_tile = gate_weight[0]
    up_tile = up_weight[0]
    down_tile = down_weight[0]
    axis_count = lax.axis_size("gx")
    column_groups = axis_count // XS
    low_bits = XS.bit_length() - 1
    high_bits = column_groups.bit_length() - 1
    device_index = lax.axis_index("gx")
    joined = tokens
    for high_step in range(high_bits):
        bit_number = low_bits + high_step
        partner_piece = from_partner(joined, "gx", bit_number)
        joined = jnp.where(
            bit_clear(device_index, bit_number),
            jnp.concatenate([joined, partner_piece], axis=1),
            jnp.concatenate([partner_piece, joined], axis=1),
        )
    gate_part = jnp.dot(joined, gate_tile, preferred_element_type=jnp.float32)
    up_part = jnp.dot(joined, up_tile, preferred_element_type=jnp.float32)
    stacked = jnp.stack([gate_part, up_part])
    for bit_number in range(low_bits - 1, -1, -1):
        half_width = stacked.shape[2] // 2
        lower_half = stacked[:, :, :half_width]
        upper_half = stacked[:, :, half_width:]
        keep_lower = bit_clear(device_index, bit_number)
        outgoing = jnp.where(keep_lower, upper_half, lower_half)
        kept_half = jnp.where(keep_lower, lower_half, upper_half)
        stacked = kept_half + from_partner(outgoing.astype(jnp.bfloat16), "gx", bit_number).astype(
            outgoing.dtype
        )
    hidden = (jax.nn.gelu(stacked[0], approximate=True) * stacked[1]).astype(jnp.bfloat16)
    hidden_joined = hidden
    for high_step in range(high_bits):
        bit_number = low_bits + high_step
        partner_hidden = from_partner(hidden_joined, "gx", bit_number)
        hidden_joined = jnp.where(
            bit_clear(device_index, bit_number),
            jnp.concatenate([hidden_joined, partner_hidden], axis=1),
            jnp.concatenate([partner_hidden, hidden_joined], axis=1),
        )
    partial_value = jnp.dot(hidden_joined, down_tile, preferred_element_type=jnp.float32)
    for bit_number in range(low_bits - 1, -1, -1):
        half_width = partial_value.shape[1] // 2
        lower_half = partial_value[:, :half_width]
        upper_half = partial_value[:, half_width:]
        keep_lower = bit_clear(device_index, bit_number)
        outgoing = jnp.where(keep_lower, upper_half, lower_half)
        kept_half = jnp.where(keep_lower, lower_half, upper_half)
        partial_value = kept_half + from_partner(
            outgoing.astype(jnp.bfloat16), "gx", bit_number
        ).astype(outgoing.dtype)
    return partial_value.astype(jnp.bfloat16)


def tile_of(width):
    for tiles in range(1, width // 128 + 1):
        if width % tiles == 0 and (width // tiles) % 128 == 0 and width // tiles <= 2304:
            return width // tiles
    return 128


def gelu(v):
    return 0.5 * v * (1.0 + jnp.tanh(0.7978845608 * (v + 0.044715 * (v * v * v))))


def kernel(
    plan, halves, tok_t, gate, up, down, out_t,
    raw, tok, tok_in, joined, wts, wd, sib_out, sib_in, z1_out, y1_out, z2_out, y2_out,
    z1_in, y1_in, z2_in, y2_in, keep_z, keep_y, keep_o, hid, hid_in,
    acc, blocks, keep_d, dsib_out, dsib_in, dout, din, done,
    raw_sem, tok_s, tok_r, w_sem, wd_sem, sib_s, sib_r, z1_s, z1_r, y1_s, y1_r,
    z2_s, z2_r, y2_s, y2_r, hid_s, hid_r, dsib_s, dsib_r, dout_s, dout_r, out_sem,
):
    bf16, f32 = jnp.bfloat16, jnp.float32
    me = lax.axis_index("gx")
    c, yb, zb, a = me % 2, (me // 2) % 2, (me // 4) % 2, me // 8
    chunks = len(plan)
    starts = [sum(plan[:s]) for s in range(chunks)]
    others = [rows - z for rows, z in zip(plan, halves)]
    z_starts = [sum(halves[:s]) for s in range(chunks)]
    y_starts = [sum(others[:s]) for s in range(chunks)]
    feat, count = raw.shape
    width = hid.shape[1]
    col = tile_of(width)
    ncol = width // col
    to_c = me + 1 - 2 * c
    to_y = me + 2 - 4 * yb
    to_z = me + 4 - 8 * zb
    to_d = me + 2 - 4 * yb + 4 - 8 * zb
    to_a = me + 8 - 16 * a

    def span(s):
        return pl.ds(starts[s], plan[s])

    def z_span(s):
        return pl.ds(z_starts[s], halves[s])

    def y_span(s):
        return pl.ds(y_starts[s], others[s])

    def block_of(kind, core):
        zz = 1 - zb if kind in (DIAG, ZN) else zb
        yy = 1 - yb if kind in (DIAG, YN) else yb
        return zz * 4 + yy * 2 + core

    def remote(src, dst, ss, rs, target):
        return pltpu.make_async_remote_copy(
            src_ref=src, dst_ref=dst, send_sem=ss, recv_sem=rs,
            device_id={"gx": target}, device_id_type=MESH,
        )

    def weight_copies(slot):
        block = block_of(slot // 2, 1 - c if slot % 2 == 0 else c)
        cols = pl.ds(pl.multiple_of(block * width, 128), width)
        return [
            pltpu.make_async_copy(w.at[0, :, cols], wts.at[i, slot], w_sem.at[i, slot])
            for i, w in ((0, gate), (1, up))
        ]

    raw_copy = pltpu.make_async_copy(tok_t, raw, raw_sem)
    raw_copy.start()
    barrier = pltpu.get_barrier_semaphore()
    for target in (to_a, to_d, to_z, to_y, to_c):
        pl.semaphore_signal(barrier, inc=1, device_id={"gx": target}, device_id_type=MESH)
    order = [0, 2, 4, 1, 6, 3, 5, 7]
    for slot in order:
        for copy in weight_copies(slot):
            copy.start()
    down_copy = pltpu.make_async_copy(down.at[0], wd, wd_sem)
    down_copy.start()
    raw_copy.wait()
    for first in range(0, count, 128):
        tok[first:first + 128, :] = raw[:, first:first + 128].T
    pl.semaphore_wait(barrier, 5)

    def tok_copy(s):
        r = span(s)
        return remote(tok.at[r], tok_in.at[r], tok_s.at[s], tok_r.at[s], to_a)

    def join(s):
        tok_copy(s).wait_recv()
        if s + 1 < chunks:
            tok_copy(s + 1).start()
        r = span(s)

        @pl.when(a == 0)
        def _():
            joined[r, 0:feat] = tok[r, :]
            joined[r, feat:2 * feat] = tok_in[r, :]

        @pl.when(a == 1)
        def _():
            joined[r, 0:feat] = tok_in[r, :]
            joined[r, feat:2 * feat] = tok[r, :]

    def each_tile(s, slot, body):
        if s == 0:
            for copy in weight_copies(slot):
                copy.wait()
        lhs = joined.at[span(s), :]

        def step(t, carry):
            g = t // ncol
            cols = pl.ds(pl.multiple_of((t % ncol) * col, 128), col)
            part = jnp.dot(lhs[...], wts[g, slot, :, cols], preferred_element_type=f32)
            body(g, cols, part)
            return carry

        lax.fori_loop(0, 2 * ncol, step, 0)

    def sib_copy(s, kind):
        return remote(
            sib_out.at[kind, :, pl.ds(0, plan[s])], sib_in.at[kind, :, span(s)],
            sib_s.at[s, kind], sib_r.at[s, kind], to_c,
        )

    def sibling(s, kind):
        if s > 0:
            sib_copy(s - 1, kind).wait_send()

        def body(g, cols, part):
            sib_out[kind, g, 0:plan[s], cols] = part.astype(bf16)

        each_tile(s, 2 * kind, body)
        sib_copy(s, kind).start()

    def z1_copy(s, piece):
        return remote(
            z1_out.at[s % 2, piece, :, pl.ds(0, halves[s])], z1_in.at[piece, :, z_span(s)],
            z1_s.at[s, piece], z1_r.at[s, piece], to_z,
        )

    def y1_copy(s, piece):
        return remote(
            y1_out.at[s % 2, piece, :, pl.ds(0, others[s])], y1_in.at[piece, :, y_span(s)],
            y1_s.at[s, piece], y1_r.at[s, piece], to_y,
        )

    def z2_copy(s):
        return remote(
            z2_out.at[s % 2, :, pl.ds(0, others[s])], z2_in.at[:, y_span(s)], z2_s.at[s], z2_r.at[s], to_z
        )

    def y2_copy(s):
        return remote(
            y2_out.at[s % 2, :, pl.ds(0, halves[s])], y2_in.at[:, z_span(s)], y2_s.at[s], y2_r.at[s], to_y
        )

    def own(s, kind):
        k = s % 2
        h0, h1 = halves[s], others[s]
        if s >= 2 and kind in (DIAG, ZN):
            z1_copy(s - 2, kind).wait_send()
        if s >= 2 and kind in (DIAG, YN):
            y1_copy(s - 2, 0 if kind == DIAG else 1).wait_send()
        sib_copy(s, kind).wait_recv()

        def body(g, cols, part):
            total = part + sib_in[kind, g, span(s), cols].astype(f32)
            if kind == DIAG:
                z1_out[k, 0, g, 0:h0, cols] = total[:h0].astype(bf16)
                y1_out[k, 0, g, 0:h1, cols] = total[h0:].astype(bf16)
            elif kind == ZN:
                z1_out[k, 1, g, 0:h0, cols] = total[:h0].astype(bf16)
                keep_z[k, g, 0:h1, cols] = total[h0:]
            elif kind == YN:
                y1_out[k, 1, g, 0:h1, cols] = total[h0:].astype(bf16)
                keep_y[k, g, 0:h0, cols] = total[:h0]
            else:
                keep_o[g, 0:h0 + h1, cols] = total

        each_tile(s, 2 * kind + 1, body)
        if kind == DIAG:
            z1_copy(s, 0).start()
            y1_copy(s, 0).start()
        elif kind == ZN:
            z1_copy(s, 1).start()
        elif kind == YN:
            y1_copy(s, 1).start()

    def loop_cols(body):
        def step(t, carry):
            body(t // ncol, pl.ds(pl.multiple_of((t % ncol) * col, 128), col))
            return carry

        lax.fori_loop(0, 2 * ncol, step, 0)

    def relay(s):
        k = s % 2
        h0, h1 = halves[s], others[s]
        if s >= 2:
            y2_copy(s - 2).wait_send()
            z2_copy(s - 2).wait_send()
        z1_copy(s, 0).wait_recv()

        def to_y2(g, cols):
            total = keep_y[k, g, 0:h0, cols] + z1_in[0, g, z_span(s), cols].astype(f32)
            y2_out[k, g, 0:h0, cols] = total.astype(bf16)

        loop_cols(to_y2)
        y2_copy(s).start()
        y1_copy(s, 0).wait_recv()

        def to_z2(g, cols):
            total = keep_z[k, g, 0:h1, cols] + y1_in[0, g, y_span(s), cols].astype(f32)
            z2_out[k, g, 0:h1, cols] = total.astype(bf16)

        loop_cols(to_z2)
        z2_copy(s).start()

    def hid_copy(s):
        r = span(s)
        return remote(hid.at[r], hid_in.at[r], hid_s.at[s], hid_r.at[s], to_a)

    def finish(s):
        own(s, OWN)
        z1_copy(s, 1).wait_recv()
        y1_copy(s, 1).wait_recv()
        y2_copy(s).wait_recv()
        z2_copy(s).wait_recv()
        h0, rows = halves[s], plan[s]

        def step(t, carry):
            cols = pl.ds(pl.multiple_of(t * col, 128), col)
            for low, high, first, second in (
                (0, h0, z1_in.at[1, :, z_span(s)], y2_in.at[:, z_span(s)]),
                (h0, rows, y1_in.at[1, :, y_span(s)], z2_in.at[:, y_span(s)]),
            ):
                g, u = (
                    keep_o[i, low:high, cols] + first[i, :, cols].astype(f32) + second[i, :, cols].astype(f32)
                    for i in (0, 1)
                )
                hid[pl.ds(starts[s] + low, high - low), cols] = (gelu(g) * u).astype(bf16)
            return carry

        lax.fori_loop(0, ncol, step, 0)
        hid_copy(s).start()

    full = acc.shape[1]
    dcol = tile_of(full)
    dwidth = blocks.shape[2]

    def dsib_copy(s, kind):
        r = span(s)
        return remote(
            dsib_out.at[kind, r], dsib_in.at[kind, r], dsib_s.at[s, kind], dsib_r.at[s, kind], to_c
        )

    def dout_copy(s, kind):
        r = span(s)
        target = (to_d, to_z, to_y)[kind]
        return remote(dout.at[kind, r], din.at[kind, r], dout_s.at[s, kind], dout_r.at[s, kind], target)

    def project(s):
        rows = plan[s]
        if s == 0:
            down_copy.wait()
        first = pl.ds(pl.multiple_of(a * width, 128), width)
        second = pl.ds(pl.multiple_of((1 - a) * width, 128), width)
        mine, theirs = hid.at[span(s), :], hid_in.at[span(s), :]

        def own_half(t, carry):
            cols = pl.ds(pl.multiple_of(t * dcol, 128), dcol)
            acc[0:rows, cols] = jnp.dot(mine[...], wd[first, cols], preferred_element_type=f32)
            return carry

        lax.fori_loop(0, full // dcol, own_half, 0)
        hid_copy(s).wait_recv()

        def other_half(t, carry):
            cols = pl.ds(pl.multiple_of(t * dcol, 128), dcol)
            acc[0:rows, cols] += jnp.dot(theirs[...], wd[second, cols], preferred_element_type=f32)
            return carry

        lax.fori_loop(0, full // dcol, other_half, 0)
        for b in range(XS):
            blocks[b, 0:rows] = acc[0:rows, b * dwidth:(b + 1) * dwidth]
        for kind in range(4):
            dsib_out[kind, span(s)] = blocks[block_of(kind, 1 - c), 0:rows].astype(bf16)
            dsib_copy(s, kind).start()

    def spread(s):
        for kind in range(4):
            dsib_copy(s, kind).wait_recv()
            total = blocks[block_of(kind, c), 0:plan[s]] + dsib_in[kind, span(s)].astype(f32)
            if kind == OWN:
                keep_d[span(s)] = total
            else:
                dout[kind, span(s)] = total.astype(bf16)

    def send_out(s):
        for kind in range(3):
            dout_copy(s, kind).start()

    def collect(s):
        total = keep_d[span(s)]
        for kind in range(3):
            dout_copy(s, kind).wait_recv()
            total = total + din[kind, span(s)].astype(f32)
        keep_d[span(s)] = total

    last = chunks - 1
    tok_copy(0).start()
    join(0)
    for kind in (DIAG, ZN, YN):
        sibling(0, kind)
    own(0, DIAG)
    sibling(0, OWN)
    own(0, ZN)
    own(0, YN)
    projected = 0
    for s in range(chunks):
        if s > 0:
            for kind in range(3):
                own(s, kind)
        if s < last:
            join(s + 1)
            for kind in range(4):
                sibling(s + 1, kind)
        if s >= 3:
            project(projected)
        if s > 0:
            finish(s - 1)
        if s >= 3:
            spread(projected)
            projected += 1
        relay(s)
    for s in range(projected):
        send_out(s)
    while projected < last:
        project(projected)
        if projected == last - 2 or last < 2:
            finish(last)
        spread(projected)
        send_out(projected)
        projected += 1
    project(last)
    spread(last)
    send_out(last)
    for s in range(chunks):
        collect(s)
    for first in range(0, count, 128):
        done[:, first:first + 128] = keep_d[first:first + 128, :].T.astype(bf16)
    out_copy = pltpu.make_async_copy(done, out_t, out_sem)
    out_copy.start()

    for s in range(chunks):
        tok_copy(s).wait_send()
        hid_copy(s).wait_send()
        for kind in range(4):
            if s == last:
                sib_copy(s, kind).wait_send()
            dsib_copy(s, kind).wait_send()
        for kind in range(3):
            dout_copy(s, kind).wait_send()
        if s >= chunks - 2:
            for piece in range(2):
                z1_copy(s, piece).wait_send()
                y1_copy(s, piece).wait_send()
            z2_copy(s).wait_send()
            y2_copy(s).wait_send()
    out_copy.wait()


def plan_of(count):
    unit = count // sum(PLAN)
    plan = [unit * parts for parts in PLAN]
    halves = [unit // 2 * parts for parts in Z_ROWS]
    return plan, halves


def fused(tokens, gate_weight, up_weight, down_weight):
    count, feat = tokens.shape
    depth, half = gate_weight.shape[1:]
    deep, full = down_weight.shape[1:]
    width, dwidth = half // XS, full // XS
    plan, halves = plan_of(count)
    others = [rows - z for rows, z in zip(plan, halves)]
    rows, h0, h1 = max(plan), max(halves), max(others)
    all0, all1 = sum(halves), sum(others)
    bf16, f32 = jnp.bfloat16, jnp.float32
    v = pltpu.VMEM
    buffers = [
        v((feat, count), bf16),
        v((count, feat), bf16),
        v((count, feat), bf16),
        v((count, 2 * feat), bf16),
        v((2, XS, depth, width), bf16),
        v((deep, full), bf16),
        v((4, 2, rows, width), bf16),
        v((4, 2, count, width), bf16),
        v((2, 2, 2, h0, width), bf16),
        v((2, 2, 2, h1, width), bf16),
        v((2, 2, h1, width), bf16),
        v((2, 2, h0, width), bf16),
        v((2, 2, all0, width), bf16),
        v((2, 2, all1, width), bf16),
        v((2, all1, width), bf16),
        v((2, all0, width), bf16),
        v((2, 2, h1, width), f32),
        v((2, 2, h0, width), f32),
        v((2, rows, width), f32),
        v((count, width), bf16),
        v((count, width), bf16),
        v((rows, full), f32),
        v((XS, rows, dwidth), f32),
        v((count, dwidth), f32),
        v((4, count, dwidth), bf16),
        v((4, count, dwidth), bf16),
        v((3, count, dwidth), bf16),
        v((3, count, dwidth), bf16),
        v((dwidth, count), bf16),
    ]
    sem = pltpu.SemaphoreType.DMA
    s = len(plan)
    shapes = [None, (s,), (s,), (2, XS), None, (s, 4), (s, 4), (s, 2), (s, 2), (s, 2), (s, 2)]
    shapes += [(s,)] * 6 + [(s, 4), (s, 4), (s, 3), (s, 3), None]
    sems = [sem if shape is None else sem(shape) for shape in shapes]
    hbm = pl.BlockSpec(memory_space=pl.ANY)
    result = pl.pallas_call(
        functools.partial(kernel, plan, halves),
        out_shape=jax.ShapeDtypeStruct((dwidth, count), bf16),
        in_specs=[hbm, hbm, hbm, hbm],
        out_specs=hbm,
        scratch_shapes=buffers + sems,
        compiler_params=pltpu.CompilerParams(
            collective_id=0, has_side_effects=True, vmem_limit_bytes=VMEM_BYTES
        ),
    )(tokens.T, gate_weight, up_weight, down_weight)
    return result.T


def shards(tokens, gate_weight, up_weight, down_weight):
    width = gate_weight.shape[2] // XS
    suits = (
        lax.axis_size("gx") == 2 * XS
        and width % 128 == 0
        and down_weight.shape[2] % 128 == 0
        and tokens.shape[0] % (32 * sum(PLAN)) == 0
        and tokens.shape[0] % 128 == 0
        and tokens.shape[1] % 16 == 0
        and tokens.shape[1] == down_weight.shape[2] // XS
    )
    if suits:
        return fused(tokens, gate_weight, up_weight, down_weight)
    return plain_shards(tokens, gate_weight, up_weight, down_weight)


def solution(mesh):
    placed = (P("groups", "gx"), P("gx", None, None), P("gx", None, None), P("gx", None, None))
    return jax.shard_map(
        shards, mesh=mesh, in_specs=placed, out_specs=P("groups", "gx"), check_vma=False
    )
```

```python
import functools

import jax
import jax.numpy as jnp
from jax import lax
from jax.experimental import pallas as pl
from jax.experimental.pallas import tpu as pltpu
from jax.sharding import PartitionSpec as P

XS = 8
PLAN = (4, 7, 6, 5, 2)
Z_ROWS = (2, 2, 2, 1, 0)
RELAYED = 3
Z_FIRST = True
VMEM_BYTES = 67043328
MESH = pl.DeviceIdType.MESH
DIAG, ZN, YN, OWN = 0, 1, 2, 3


def from_partner(block, axis, bit):
    count = lax.axis_size(axis)
    route = []
    for low in range(count):
        high = low | 1 << bit
        if high != low and high < count:
            route += [(low, high), (high, low)]
    return lax.ppermute(block, axis, route)


def bit_clear(device_index, bit_number):
    return device_index >> bit_number & 1 == 0


def plain_shards(tokens, gate_weight, up_weight, down_weight):
    gate_tile = gate_weight[0]
    up_tile = up_weight[0]
    down_tile = down_weight[0]
    axis_count = lax.axis_size("gx")
    column_groups = axis_count // XS
    low_bits = XS.bit_length() - 1
    high_bits = column_groups.bit_length() - 1
    device_index = lax.axis_index("gx")
    joined = tokens
    for high_step in range(high_bits):
        bit_number = low_bits + high_step
        partner_piece = from_partner(joined, "gx", bit_number)
        joined = jnp.where(
            bit_clear(device_index, bit_number),
            jnp.concatenate([joined, partner_piece], axis=1),
            jnp.concatenate([partner_piece, joined], axis=1),
        )
    gate_part = jnp.dot(joined, gate_tile, preferred_element_type=jnp.float32)
    up_part = jnp.dot(joined, up_tile, preferred_element_type=jnp.float32)
    stacked = jnp.stack([gate_part, up_part])
    for bit_number in range(low_bits - 1, -1, -1):
        half_width = stacked.shape[2] // 2
        lower_half = stacked[:, :, :half_width]
        upper_half = stacked[:, :, half_width:]
        keep_lower = bit_clear(device_index, bit_number)
        outgoing = jnp.where(keep_lower, upper_half, lower_half)
        kept_half = jnp.where(keep_lower, lower_half, upper_half)
        stacked = kept_half + from_partner(outgoing.astype(jnp.bfloat16), "gx", bit_number).astype(
            outgoing.dtype
        )
    hidden = (jax.nn.gelu(stacked[0], approximate=True) * stacked[1]).astype(jnp.bfloat16)
    hidden_joined = hidden
    for high_step in range(high_bits):
        bit_number = low_bits + high_step
        partner_hidden = from_partner(hidden_joined, "gx", bit_number)
        hidden_joined = jnp.where(
            bit_clear(device_index, bit_number),
            jnp.concatenate([hidden_joined, partner_hidden], axis=1),
            jnp.concatenate([partner_hidden, hidden_joined], axis=1),
        )
    partial_value = jnp.dot(hidden_joined, down_tile, preferred_element_type=jnp.float32)
    for bit_number in range(low_bits - 1, -1, -1):
        half_width = partial_value.shape[1] // 2
        lower_half = partial_value[:, :half_width]
        upper_half = partial_value[:, half_width:]
        keep_lower = bit_clear(device_index, bit_number)
        outgoing = jnp.where(keep_lower, upper_half, lower_half)
        kept_half = jnp.where(keep_lower, lower_half, upper_half)
        partial_value = kept_half + from_partner(
            outgoing.astype(jnp.bfloat16), "gx", bit_number
        ).astype(outgoing.dtype)
    return partial_value.astype(jnp.bfloat16)


def tile_of(width):
    for tiles in range(1, width // 128 + 1):
        if width % tiles == 0 and (width // tiles) % 128 == 0 and width // tiles <= 2304:
            return width // tiles
    return 128


def gelu(v):
    return 0.5 * v * (1.0 + jnp.tanh(0.7978845608 * (v + 0.044715 * (v * v * v))))


def kernel(
    plan, halves, tok_t, gate, up, down, out_t,
    raw, tok, tok_in, joined, wts, wd, sib_out, sib_in, z1_out, y1_out, z2_out, y2_out,
    z1_in, y1_in, z2_in, y2_in, keep_z, keep_y, keep_o, hid, hid_in,
    acc, blocks, keep_d, keep_n, dsib_out, dsib_in, dout, din, done,
    raw_sem, tok_s, tok_r, w_sem, wd_sem, sib_s, sib_r, z1_s, z1_r, y1_s, y1_r,
    z2_s, z2_r, y2_s, y2_r, hid_s, hid_r, dsib_s, dsib_r, dout_s, dout_r, out_sem,
):
    bf16, f32 = jnp.bfloat16, jnp.float32
    me = lax.axis_index("gx")
    c, yb, zb, a = me % 2, (me // 2) % 2, (me // 4) % 2, me // 8
    chunks = len(plan)
    last = chunks - 1
    starts = [sum(plan[:s]) for s in range(chunks)]
    others = [rows - z for rows, z in zip(plan, halves)]
    z_starts = [sum(halves[:s]) for s in range(chunks)]
    y_starts = [sum(others[:s]) for s in range(chunks)]
    feat, count = raw.shape
    width = hid.shape[1]
    col = tile_of(width)
    ncol = width // col
    to_c = me + 1 - 2 * c
    to_y = me + 2 - 4 * yb
    to_z = me + 4 - 8 * zb
    to_d = me + 2 - 4 * yb + 4 - 8 * zb
    to_a = me + 8 - 16 * a

    def span(s):
        return pl.ds(starts[s], plan[s])

    def z_span(s):
        return pl.ds(z_starts[s], halves[s])

    def y_span(s):
        return pl.ds(y_starts[s], others[s])

    def block_of(kind, core):
        zz = 1 - zb if kind in (DIAG, ZN) else zb
        yy = 1 - yb if kind in (DIAG, YN) else yb
        return zz * 4 + yy * 2 + core

    def remote(src, dst, ss, rs, target):
        return pltpu.make_async_remote_copy(
            src_ref=src, dst_ref=dst, send_sem=ss, recv_sem=rs,
            device_id={"gx": target}, device_id_type=MESH,
        )

    def weight_copies(slot):
        block = block_of(slot // 2, 1 - c if slot % 2 == 0 else c)
        cols = pl.ds(pl.multiple_of(block * width, 128), width)
        return [
            pltpu.make_async_copy(w.at[0, :, cols], wts.at[i, slot], w_sem.at[slot])
            for i, w in ((0, gate), (1, up))
        ]

    raw_copy = pltpu.make_async_copy(tok_t, raw, raw_sem)
    raw_copy.start()
    barrier = pltpu.get_barrier_semaphore()
    for target in (to_a, to_d, to_z, to_y, to_c):
        pl.semaphore_signal(barrier, inc=1, device_id={"gx": target}, device_id_type=MESH)
    order = [0, 2, 4, 1, 6, 3, 5, 7]
    for slot in order:
        for copy in weight_copies(slot):
            copy.start()
    down_copy = pltpu.make_async_copy(down.at[0], wd, wd_sem)
    down_copy.start()
    raw_copy.wait()
    for first in range(0, count, 128):
        tok[first:first + 128, :] = raw[:, first:first + 128].T
    pl.semaphore_wait(barrier, 5)

    def tok_copy(s):
        r = span(s)
        return remote(tok.at[r], tok_in.at[r], tok_s, tok_r.at[s], to_a)

    def join(s):
        tok_copy(s).wait_recv()
        if s + 1 < chunks:
            tok_copy(s + 1).start()
        r = span(s)

        @pl.when(a == 0)
        def _():
            joined[r, 0:feat] = tok[r, :]
            joined[r, feat:2 * feat] = tok_in[r, :]

        @pl.when(a == 1)
        def _():
            joined[r, 0:feat] = tok_in[r, :]
            joined[r, feat:2 * feat] = tok[r, :]

    def each_tile(s, slot, body):
        if s == 0:
            both = wts.at[:, slot]
            pltpu.make_async_copy(both, both, w_sem.at[slot]).wait()
        lhs = joined.at[span(s), :]

        def step(t, carry):
            g = t // ncol
            cols = pl.ds(pl.multiple_of((t % ncol) * col, 128), col)
            part = jnp.dot(lhs[...], wts[g, slot, :, cols], preferred_element_type=f32)
            body(g, cols, part)
            return carry

        lax.fori_loop(0, 2 * ncol, step, 0)

    def sib_copy(s, kind):
        if s == 0:
            return remote(
                sib_out.at[kind, :, pl.ds(0, plan[s])], sib_in.at[kind, :, span(s)],
                sib_s.at[kind], sib_r.at[kind], to_c,
            )
        return remote(
            sib_out.at[:, :, pl.ds(0, plan[s])], sib_in.at[:, :, span(s)], sib_s.at[4], sib_r.at[3 + s], to_c
        )

    def sibling(s, kind):
        if s == 1:
            sib_copy(0, kind).wait_send()
        elif s > 1 and kind == 0:
            sib_copy(s - 1, kind).wait_send()

        def body(g, cols, part):
            sib_out[kind, g, 0:plan[s], cols] = part.astype(bf16)

        each_tile(s, 2 * kind, body)
        if s == 0 or kind == 3:
            sib_copy(s, kind).start()

    def z1_copy(s, piece):
        return remote(
            z1_out.at[s % 2, piece, :, pl.ds(0, halves[s])], z1_in.at[piece, :, z_span(s)],
            z1_s.at[s % 2, piece], z1_r.at[s, piece], to_z,
        )

    def y1_copy(s, piece):
        return remote(
            y1_out.at[s % 2, piece, :, pl.ds(0, others[s])], y1_in.at[piece, :, y_span(s)],
            y1_s.at[s % 2, piece], y1_r.at[s, piece], to_y,
        )

    def z2_copy(s):
        return remote(
            z2_out.at[s % 2, :, pl.ds(0, others[s])], z2_in.at[:, y_span(s)], z2_s.at[s % 2], z2_r.at[s], to_z
        )

    def y2_copy(s):
        return remote(
            y2_out.at[s % 2, :, pl.ds(0, halves[s])], y2_in.at[:, z_span(s)], y2_s.at[s % 2], y2_r.at[s], to_y
        )

    def own(s, kind):
        k = s % 2
        h0, h1 = halves[s], others[s]
        if s >= 2 and kind in (DIAG, ZN) and halves[s - 2]:
            z1_copy(s - 2, kind).wait_send()
        if s >= 2 and kind in (DIAG, YN):
            y1_copy(s - 2, 0 if kind == DIAG else 1).wait_send()
        if s == 0 or kind == 0:
            sib_copy(s, kind).wait_recv()

        def body(g, cols, part):
            total = part + sib_in[kind, g, span(s), cols].astype(f32)
            if kind == DIAG:
                if h0:
                    z1_out[k, 0, g, 0:h0, cols] = total[:h0].astype(bf16)
                y1_out[k, 0, g, 0:h1, cols] = total[h0:].astype(bf16)
            elif kind == ZN:
                if h0:
                    z1_out[k, 1, g, 0:h0, cols] = total[:h0].astype(bf16)
                keep_z[k, g, 0:h1, cols] = total[h0:]
            elif kind == YN:
                y1_out[k, 1, g, 0:h1, cols] = total[h0:].astype(bf16)
                if h0:
                    keep_y[k, g, 0:h0, cols] = total[:h0]
            else:
                keep_o[g, 0:h0 + h1, cols] = total

        each_tile(s, 2 * kind + 1, body)
        if h0 and kind in (DIAG, ZN):
            z1_copy(s, kind).start()
        if kind == DIAG:
            y1_copy(s, 0).start()
        elif kind == YN:
            y1_copy(s, 1).start()

    def loop_cols(body):
        def step(t, carry):
            body(t // ncol, pl.ds(pl.multiple_of((t % ncol) * col, 128), col))
            return carry

        lax.fori_loop(0, 2 * ncol, step, 0)

    def relay_y(s):
        k, h0 = s % 2, halves[s]
        if s >= 2 and halves[s - 2]:
            y2_copy(s - 2).wait_send()
        if h0 == 0:
            return
        z1_copy(s, 0).wait_recv()

        def to_y2(g, cols):
            total = keep_y[k, g, 0:h0, cols] + z1_in[0, g, z_span(s), cols].astype(f32)
            y2_out[k, g, 0:h0, cols] = total.astype(bf16)

        loop_cols(to_y2)
        y2_copy(s).start()

    def relay_z(s):
        k, h1 = s % 2, others[s]
        if s >= 2:
            z2_copy(s - 2).wait_send()
        y1_copy(s, 0).wait_recv()

        def to_z2(g, cols):
            total = keep_z[k, g, 0:h1, cols] + y1_in[0, g, y_span(s), cols].astype(f32)
            z2_out[k, g, 0:h1, cols] = total.astype(bf16)

        loop_cols(to_z2)
        z2_copy(s).start()

    def relay(s):
        for step in (relay_z, relay_y) if Z_FIRST else (relay_y, relay_z):
            step(s)

    def hid_copy(s):
        r = span(s)
        return remote(hid.at[r], hid_in.at[r], hid_s, hid_r.at[s], to_a)

    def finish(s):
        own(s, OWN)
        y1_copy(s, 1).wait_recv()
        if halves[s]:
            z1_copy(s, 1).wait_recv()
            y2_copy(s).wait_recv()
        z2_copy(s).wait_recv()
        h0, rows = halves[s], plan[s]

        def step(t, carry):
            cols = pl.ds(pl.multiple_of(t * col, 128), col)
            pieces = [(h0, rows, y1_in.at[1, :, y_span(s)], z2_in.at[:, y_span(s)])]
            if h0:
                pieces.append((0, h0, z1_in.at[1, :, z_span(s)], y2_in.at[:, z_span(s)]))
            for low, high, first, second in pieces:
                g, u = (
                    keep_o[i, low:high, cols] + first[i, :, cols].astype(f32) + second[i, :, cols].astype(f32)
                    for i in (0, 1)
                )
                hid[pl.ds(starts[s] + low, high - low), cols] = (gelu(g) * u).astype(bf16)
            return carry

        lax.fori_loop(0, ncol, step, 0)
        hid_copy(s).start()

    full = acc.shape[1]
    part = full // 2
    dwidth = blocks.shape[2]

    def dsib_copy(s, side):
        near = pl.ds(2 * side, 2)
        r = span(s)
        return remote(dsib_out.at[near, r], dsib_in.at[near, r], dsib_s, dsib_r.at[s, side], to_c)

    def dout_copy(s, kind):
        r = span(s)
        target = (to_y if s < RELAYED else to_d, to_z, to_y)[kind]
        return remote(dout.at[kind, r], din.at[kind, r], dout_s, dout_r.at[s, kind], target)

    def base_of(s):
        return plan[s - 1] if s == last else 0

    def project_own(s):
        rows, base = plan[s], base_of(s)
        if s == 0:
            down_copy.wait()
        first = pl.ds(pl.multiple_of(a * width, 128), width)
        mine = hid.at[span(s), :]

        acc[base:base + rows, :] = jnp.dot(mine[...], wd[first, :], preferred_element_type=f32)

    def project_other(s):
        rows, base = plan[s], base_of(s)
        second = pl.ds(pl.multiple_of((1 - a) * width, 128), width)
        theirs = hid_in.at[span(s), :]
        hid_copy(s).wait_recv()
        for near, side in enumerate((1 - zb, zb)):
            cols = pl.ds(pl.multiple_of(side * part, 128), part)
            total = acc[base:base + rows, cols] + jnp.dot(
                theirs[...], wd[second, cols], preferred_element_type=f32
            )
            for b in range(XS // 2):
                blocks[side * (XS // 2) + b, 0:rows] = total[:, b * dwidth:(b + 1) * dwidth]
            for kind in (2 * near, 2 * near + 1):
                dsib_out[kind, span(s)] = blocks[block_of(kind, 1 - c), 0:rows].astype(bf16)
            dsib_copy(s, near).start()

    def project(s):
        project_own(s)
        project_other(s)

    def spread(s):
        for kind in (DIAG, ZN, YN, OWN):
            if kind in (DIAG, YN):
                dsib_copy(s, kind // 2).wait_recv()
            total = blocks[block_of(kind, c), 0:plan[s]] + dsib_in[kind, span(s)].astype(f32)
            if kind == OWN:
                keep_d[span(s)] = total
            elif kind == ZN and s < RELAYED:
                keep_n[span(s)] = total
            else:
                dout[kind, span(s)] = total.astype(bf16)

    def send_out(s):
        for kind in (DIAG, YN) if s < RELAYED else (DIAG, YN, ZN):
            dout_copy(s, kind).start()

    def relay_out(s):
        dout_copy(s, DIAG).wait_recv()
        total = keep_n[span(s)] + din[DIAG, span(s)].astype(f32)
        dout[ZN, span(s)] = total.astype(bf16)
        dout_copy(s, ZN).start()

    def relay_outs(s):
        if s < RELAYED:
            relay_out(s)

    def collect(s):
        total = keep_d[span(s)]
        for kind in (YN, ZN) if s < RELAYED else (YN, ZN, DIAG):
            dout_copy(s, kind).wait_recv()
            total = total + din[kind, span(s)].astype(f32)
        keep_d[span(s)] = total

    tok_copy(0).start()
    join(0)
    sibling(0, DIAG)
    sibling(0, ZN)
    own(0, DIAG)
    sibling(0, YN)
    own(0, ZN)
    sibling(0, OWN)
    own(0, YN)
    for s in range(chunks):
        if s > 0:
            for kind in range(3):
                own(s, kind)
        if s < last:
            join(s + 1)
            for kind in range(4):
                sibling(s + 1, kind)
        if s >= 3:
            project(s - 3)
        if s > 0:
            finish(s - 1)
        if s >= 3:
            spread(s - 3)
        relay(s)
    for s in range(last - 2):
        send_out(s)
    project(last - 2)
    project_own(last - 1)
    for s in range(last - 3):
        relay_outs(s)
    finish(last)
    spread(last - 2)
    send_out(last - 2)
    relay_outs(last - 3)
    project_other(last - 1)
    project_own(last)
    spread(last - 1)
    send_out(last - 1)
    relay_outs(last - 2)
    project_other(last)
    spread(last)
    send_out(last)
    for s in range(chunks):
        collect(s)
    for first in range(0, count, 128):
        done[:, first:first + 128] = keep_d[first:first + 128, :].T.astype(bf16)
    out_copy = pltpu.make_async_copy(done, out_t, out_sem)
    out_copy.start()

    for buffer, sem, target in (
        (tok, tok_s, to_a), (hid, hid_s, to_a), (dsib_out, dsib_s, to_c), (dout, dout_s, to_y)
    ):
        remote(buffer, buffer, sem, out_sem, target).wait_send()
    sib_copy(last, 0).wait_send()
    for s in range(max(chunks - 2, 0), chunks):
        for piece in range(2):
            if halves[s]:
                z1_copy(s, piece).wait_send()
            y1_copy(s, piece).wait_send()
        z2_copy(s).wait_send()
        if halves[s]:
            y2_copy(s).wait_send()
    out_copy.wait()


def plan_of(count):
    unit = count // sum(PLAN)
    plan = [unit * parts for parts in PLAN]
    halves = [unit * parts for parts in Z_ROWS]
    return plan, halves


def fused(tokens, gate_weight, up_weight, down_weight):
    count, feat = tokens.shape
    depth, half = gate_weight.shape[1:]
    deep, full = down_weight.shape[1:]
    width, dwidth = half // XS, full // XS
    plan, halves = plan_of(count)
    others = [rows - z for rows, z in zip(plan, halves)]
    rows, h0, h1 = max(plan), max(halves), max(others)
    all0, all1 = sum(halves), sum(others)
    bf16, f32 = jnp.bfloat16, jnp.float32
    v = pltpu.VMEM
    buffers = [
        v((feat, count), bf16),
        v((count, feat), bf16),
        v((count, feat), bf16),
        v((count, 2 * feat), bf16),
        v((2, XS, depth, width), bf16),
        v((deep, full), bf16),
        v((4, 2, rows, width), bf16),
        v((4, 2, count, width), bf16),
        v((2, 2, 2, h0, width), bf16),
        v((2, 2, 2, h1, width), bf16),
        v((2, 2, h1, width), bf16),
        v((2, 2, h0, width), bf16),
        v((2, 2, all0, width), bf16),
        v((2, 2, all1, width), bf16),
        v((2, all1, width), bf16),
        v((2, all0, width), bf16),
        v((2, 2, h1, width), f32),
        v((2, 2, h0, width), f32),
        v((2, rows, width), f32),
        v((count, width), bf16),
        v((count, width), bf16),
        v((max(rows, plan[-2] + plan[-1]), full), f32),
        v((XS, rows, dwidth), f32),
        v((count, dwidth), f32),
        v((count, dwidth), f32),
        v((4, count, dwidth), bf16),
        v((4, count, dwidth), bf16),
        v((3, count, dwidth), bf16),
        v((3, count, dwidth), bf16),
        v((dwidth, count), bf16),
    ]
    sem = pltpu.SemaphoreType.DMA
    s = len(plan)
    shapes = [None, None, (s,), (XS,), None, (5,), (s + 3,), (2, 2), (s, 2), (2, 2), (s, 2)]
    shapes += [(2,), (s,), (2,), (s,), None, (s,), None, (s, 2), None, (s, 3), None]
    sems = [sem if shape is None else sem(shape) for shape in shapes]
    hbm = pl.BlockSpec(memory_space=pl.ANY)
    result = pl.pallas_call(
        functools.partial(kernel, plan, halves),
        out_shape=jax.ShapeDtypeStruct((dwidth, count), bf16),
        in_specs=[hbm, hbm, hbm, hbm],
        out_specs=hbm,
        scratch_shapes=buffers + sems,
        compiler_params=pltpu.CompilerParams(
            collective_id=0, has_side_effects=True, vmem_limit_bytes=VMEM_BYTES
        ),
    )(tokens.T, gate_weight, up_weight, down_weight)
    return result.T


def shards(tokens, gate_weight, up_weight, down_weight):
    width = gate_weight.shape[2] // XS
    suits = (
        lax.axis_size("gx") == 2 * XS
        and width % 128 == 0
        and down_weight.shape[2] % 256 == 0
        and tokens.shape[0] % (16 * sum(PLAN)) == 0
        and tokens.shape[0] % 128 == 0
        and tokens.shape[1] % 16 == 0
        and tokens.shape[1] == down_weight.shape[2] // XS
    )
    if suits:
        return fused(tokens, gate_weight, up_weight, down_weight)
    return plain_shards(tokens, gate_weight, up_weight, down_weight)


def solution(mesh):
    placed = (P("groups", "gx"), P("gx", None, None), P("gx", None, None), P("gx", None, None))
    return jax.shard_map(
        shards, mesh=mesh, in_specs=placed, out_specs=P("groups", "gx"), check_vma=False
    )
```

```python
import functools

import jax
import jax.numpy as jnp
from jax import lax
from jax.experimental import pallas as pl
from jax.experimental.pallas import tpu as pltpu
from jax.sharding import PartitionSpec as P

XS = 8
PLAN = (4, 7, 6, 5, 2)
Z_ROWS = (2, 2, 2, 1, 0)
RELAYED = 3
Z_FIRST = False
VMEM_BYTES = 67043328
MESH = pl.DeviceIdType.MESH
DIAG, ZN, YN, OWN = 0, 1, 2, 3


def from_partner(block, axis, bit):
    count = lax.axis_size(axis)
    route = []
    for low in range(count):
        high = low | 1 << bit
        if high != low and high < count:
            route += [(low, high), (high, low)]
    return lax.ppermute(block, axis, route)


def bit_clear(device_index, bit_number):
    return device_index >> bit_number & 1 == 0


def plain_shards(tokens, gate_weight, up_weight, down_weight):
    gate_tile = gate_weight[0]
    up_tile = up_weight[0]
    down_tile = down_weight[0]
    axis_count = lax.axis_size("gx")
    column_groups = axis_count // XS
    low_bits = XS.bit_length() - 1
    high_bits = column_groups.bit_length() - 1
    device_index = lax.axis_index("gx")
    joined = tokens
    for high_step in range(high_bits):
        bit_number = low_bits + high_step
        partner_piece = from_partner(joined, "gx", bit_number)
        joined = jnp.where(
            bit_clear(device_index, bit_number),
            jnp.concatenate([joined, partner_piece], axis=1),
            jnp.concatenate([partner_piece, joined], axis=1),
        )
    gate_part = jnp.dot(joined, gate_tile, preferred_element_type=jnp.float32)
    up_part = jnp.dot(joined, up_tile, preferred_element_type=jnp.float32)
    stacked = jnp.stack([gate_part, up_part])
    for bit_number in range(low_bits - 1, -1, -1):
        half_width = stacked.shape[2] // 2
        lower_half = stacked[:, :, :half_width]
        upper_half = stacked[:, :, half_width:]
        keep_lower = bit_clear(device_index, bit_number)
        outgoing = jnp.where(keep_lower, upper_half, lower_half)
        kept_half = jnp.where(keep_lower, lower_half, upper_half)
        stacked = kept_half + from_partner(outgoing.astype(jnp.bfloat16), "gx", bit_number).astype(
            outgoing.dtype
        )
    hidden = (jax.nn.gelu(stacked[0], approximate=True) * stacked[1]).astype(jnp.bfloat16)
    hidden_joined = hidden
    for high_step in range(high_bits):
        bit_number = low_bits + high_step
        partner_hidden = from_partner(hidden_joined, "gx", bit_number)
        hidden_joined = jnp.where(
            bit_clear(device_index, bit_number),
            jnp.concatenate([hidden_joined, partner_hidden], axis=1),
            jnp.concatenate([partner_hidden, hidden_joined], axis=1),
        )
    partial_value = jnp.dot(hidden_joined, down_tile, preferred_element_type=jnp.float32)
    for bit_number in range(low_bits - 1, -1, -1):
        half_width = partial_value.shape[1] // 2
        lower_half = partial_value[:, :half_width]
        upper_half = partial_value[:, half_width:]
        keep_lower = bit_clear(device_index, bit_number)
        outgoing = jnp.where(keep_lower, upper_half, lower_half)
        kept_half = jnp.where(keep_lower, lower_half, upper_half)
        partial_value = kept_half + from_partner(
            outgoing.astype(jnp.bfloat16), "gx", bit_number
        ).astype(outgoing.dtype)
    return partial_value.astype(jnp.bfloat16)


def tile_of(width):
    for tiles in range(1, width // 128 + 1):
        if width % tiles == 0 and (width // tiles) % 128 == 0 and width // tiles <= 2304:
            return width // tiles
    return 128


def gelu(v):
    return 0.5 * v * (1.0 + jnp.tanh(0.7978845608 * (v + 0.044715 * (v * v * v))))


def kernel(
    plan, halves, tok_t, gate, up, down, out_t,
    raw, tok, tok_in, joined, wts, wd, sib_out, sib_in, z1_out, y1_out, z2_out, y2_out,
    z1_in, y1_in, z2_in, y2_in, keep_z, keep_y, keep_o, hid, hid_in,
    acc, blocks, keep_d, keep_n, dsib_out, dsib_in, dout, din, done,
    raw_sem, tok_s, tok_r, w_sem, wd_sem, sib_s, sib_r, z1_s, z1_r, y1_s, y1_r,
    z2_s, z2_r, y2_s, y2_r, hid_s, hid_r, dsib_s, dsib_r, dout_s, dout_r, out_sem,
):
    bf16, f32 = jnp.bfloat16, jnp.float32
    me = lax.axis_index("gx")
    c, yb, zb, a = me % 2, (me // 2) % 2, (me // 4) % 2, me // 8
    chunks = len(plan)
    last = chunks - 1
    starts = [sum(plan[:s]) for s in range(chunks)]
    others = [rows - z for rows, z in zip(plan, halves)]
    z_starts = [sum(halves[:s]) for s in range(chunks)]
    y_starts = [sum(others[:s]) for s in range(chunks)]
    feat, count = raw.shape
    width = hid.shape[1]
    col = tile_of(width)
    ncol = width // col
    to_c = me + 1 - 2 * c
    to_y = me + 2 - 4 * yb
    to_z = me + 4 - 8 * zb
    to_d = me + 2 - 4 * yb + 4 - 8 * zb
    to_a = me + 8 - 16 * a

    def span(s):
        return pl.ds(starts[s], plan[s])

    def z_span(s):
        return pl.ds(z_starts[s], halves[s])

    def y_span(s):
        return pl.ds(y_starts[s], others[s])

    def block_of(kind, core):
        zz = 1 - zb if kind in (DIAG, ZN) else zb
        yy = 1 - yb if kind in (DIAG, YN) else yb
        return zz * 4 + yy * 2 + core

    def remote(src, dst, ss, rs, target):
        return pltpu.make_async_remote_copy(
            src_ref=src, dst_ref=dst, send_sem=ss, recv_sem=rs,
            device_id={"gx": target}, device_id_type=MESH,
        )

    def weight_copies(slot):
        block = block_of(slot // 2, 1 - c if slot % 2 == 0 else c)
        cols = pl.ds(pl.multiple_of(block * width, 128), width)
        return [
            pltpu.make_async_copy(w.at[0, :, cols], wts.at[i, slot], w_sem.at[slot])
            for i, w in ((0, gate), (1, up))
        ]

    raw_copy = pltpu.make_async_copy(tok_t, raw, raw_sem)
    raw_copy.start()
    barrier = pltpu.get_barrier_semaphore()
    for target in (to_a, to_d, to_z, to_y, to_c):
        pl.semaphore_signal(barrier, inc=1, device_id={"gx": target}, device_id_type=MESH)
    order = [0, 2, 4, 1, 6, 3, 5, 7]
    for slot in order:
        for copy in weight_copies(slot):
            copy.start()
    down_copy = pltpu.make_async_copy(down.at[0], wd, wd_sem)
    down_copy.start()
    raw_copy.wait()
    for first in range(0, count, 128):
        tok[first:first + 128, :] = raw[:, first:first + 128].T
    pl.semaphore_wait(barrier, 5)

    def tok_copy(s):
        r = span(s)
        return remote(tok.at[r], tok_in.at[r], tok_s, tok_r.at[s], to_a)

    def join(s):
        tok_copy(s).wait_recv()
        if s + 1 < chunks:
            tok_copy(s + 1).start()
        r = span(s)

        @pl.when(a == 0)
        def _():
            joined[r, 0:feat] = tok[r, :]
            joined[r, feat:2 * feat] = tok_in[r, :]

        @pl.when(a == 1)
        def _():
            joined[r, 0:feat] = tok_in[r, :]
            joined[r, feat:2 * feat] = tok[r, :]

    def each_tile(s, slot, body):
        if s == 0:
            both = wts.at[:, slot]
            pltpu.make_async_copy(both, both, w_sem.at[slot]).wait()
        lhs = joined.at[span(s), :]

        def step(t, carry):
            g = t // ncol
            cols = pl.ds(pl.multiple_of((t % ncol) * col, 128), col)
            part = jnp.dot(lhs[...], wts[g, slot, :, cols], preferred_element_type=f32)
            body(g, cols, part)
            return carry

        lax.fori_loop(0, 2 * ncol, step, 0)

    def sib_copy(s, kind):
        if s == 0:
            return remote(
                sib_out.at[kind, :, pl.ds(0, plan[s])], sib_in.at[kind, :, span(s)],
                sib_s.at[kind], sib_r.at[kind], to_c,
            )
        return remote(
            sib_out.at[:, :, pl.ds(0, plan[s])], sib_in.at[:, :, span(s)], sib_s.at[4], sib_r.at[3 + s], to_c
        )

    def sibling(s, kind):
        if s == 1:
            sib_copy(0, kind).wait_send()
        elif s > 1 and kind == 0:
            sib_copy(s - 1, kind).wait_send()

        def body(g, cols, part):
            sib_out[kind, g, 0:plan[s], cols] = part.astype(bf16)

        each_tile(s, 2 * kind, body)
        if s == 0 or kind == 3:
            sib_copy(s, kind).start()

    def z1_copy(s, piece):
        return remote(
            z1_out.at[s % 2, piece, :, pl.ds(0, halves[s])], z1_in.at[piece, :, z_span(s)],
            z1_s.at[s % 2, piece], z1_r.at[s, piece], to_z,
        )

    def y1_copy(s, piece):
        return remote(
            y1_out.at[s % 2, piece, :, pl.ds(0, others[s])], y1_in.at[piece, :, y_span(s)],
            y1_s.at[s % 2, piece], y1_r.at[s, piece], to_y,
        )

    def z2_copy(s):
        return remote(
            z2_out.at[s % 2, :, pl.ds(0, others[s])], z2_in.at[:, y_span(s)], z2_s.at[s % 2], z2_r.at[s], to_z
        )

    def y2_copy(s):
        return remote(
            y2_out.at[s % 2, :, pl.ds(0, halves[s])], y2_in.at[:, z_span(s)], y2_s.at[s % 2], y2_r.at[s], to_y
        )

    def own(s, kind):
        k = s % 2
        h0, h1 = halves[s], others[s]
        if s >= 2 and kind in (DIAG, ZN) and halves[s - 2]:
            z1_copy(s - 2, kind).wait_send()
        if s >= 2 and kind in (DIAG, YN):
            y1_copy(s - 2, 0 if kind == DIAG else 1).wait_send()
        if s == 0 or kind == 0:
            sib_copy(s, kind).wait_recv()

        def body(g, cols, part):
            total = part + sib_in[kind, g, span(s), cols].astype(f32)
            if kind == DIAG:
                if h0:
                    z1_out[k, 0, g, 0:h0, cols] = total[:h0].astype(bf16)
                y1_out[k, 0, g, 0:h1, cols] = total[h0:].astype(bf16)
            elif kind == ZN:
                if h0:
                    z1_out[k, 1, g, 0:h0, cols] = total[:h0].astype(bf16)
                keep_z[k, g, 0:h1, cols] = total[h0:]
            elif kind == YN:
                y1_out[k, 1, g, 0:h1, cols] = total[h0:].astype(bf16)
                if h0:
                    keep_y[k, g, 0:h0, cols] = total[:h0]
            else:
                keep_o[g, 0:h0 + h1, cols] = total

        each_tile(s, 2 * kind + 1, body)
        if h0 and kind in (DIAG, ZN):
            z1_copy(s, kind).start()
        if kind == DIAG:
            y1_copy(s, 0).start()
        elif kind == YN:
            y1_copy(s, 1).start()

    def loop_cols(body):
        def step(t, carry):
            body(t // ncol, pl.ds(pl.multiple_of((t % ncol) * col, 128), col))
            return carry

        lax.fori_loop(0, 2 * ncol, step, 0)

    def relay_y(s):
        k, h0 = s % 2, halves[s]
        if s >= 2 and halves[s - 2]:
            y2_copy(s - 2).wait_send()
        if h0 == 0:
            return
        z1_copy(s, 0).wait_recv()

        def to_y2(g, cols):
            total = keep_y[k, g, 0:h0, cols] + z1_in[0, g, z_span(s), cols].astype(f32)
            y2_out[k, g, 0:h0, cols] = total.astype(bf16)

        loop_cols(to_y2)
        y2_copy(s).start()

    def relay_z(s):
        k, h1 = s % 2, others[s]
        if s >= 2:
            z2_copy(s - 2).wait_send()
        y1_copy(s, 0).wait_recv()

        def to_z2(g, cols):
            total = keep_z[k, g, 0:h1, cols] + y1_in[0, g, y_span(s), cols].astype(f32)
            z2_out[k, g, 0:h1, cols] = total.astype(bf16)

        loop_cols(to_z2)
        z2_copy(s).start()

    def relay(s):
        for step in (relay_z, relay_y) if Z_FIRST else (relay_y, relay_z):
            step(s)

    def hid_copy(s):
        r = span(s)
        return remote(hid.at[r], hid_in.at[r], hid_s, hid_r.at[s], to_a)

    def finish(s):
        own(s, OWN)
        y1_copy(s, 1).wait_recv()
        if halves[s]:
            z1_copy(s, 1).wait_recv()
            y2_copy(s).wait_recv()
        z2_copy(s).wait_recv()
        h0, rows = halves[s], plan[s]

        def step(t, carry):
            cols = pl.ds(pl.multiple_of(t * col, 128), col)
            pieces = [(h0, rows, y1_in.at[1, :, y_span(s)], z2_in.at[:, y_span(s)])]
            if h0:
                pieces.append((0, h0, z1_in.at[1, :, z_span(s)], y2_in.at[:, z_span(s)]))
            for low, high, first, second in pieces:
                g, u = (
                    keep_o[i, low:high, cols] + first[i, :, cols].astype(f32) + second[i, :, cols].astype(f32)
                    for i in (0, 1)
                )
                hid[pl.ds(starts[s] + low, high - low), cols] = (gelu(g) * u).astype(bf16)
            return carry

        lax.fori_loop(0, ncol, step, 0)
        hid_copy(s).start()

    full = acc.shape[1]
    part = full // 2
    dwidth = blocks.shape[2]

    def dsib_copy(s, side):
        near = pl.ds(2 * side, 2)
        r = span(s)
        return remote(dsib_out.at[near, r], dsib_in.at[near, r], dsib_s, dsib_r.at[s, side], to_c)

    def dout_copy(s, kind):
        r = span(s)
        target = (to_y if s < RELAYED else to_d, to_z, to_y)[kind]
        return remote(dout.at[kind, r], din.at[kind, r], dout_s, dout_r.at[s, kind], target)

    def base_of(s):
        return plan[s - 1] if s == last else 0

    def project_own(s):
        rows, base = plan[s], base_of(s)
        if s == 0:
            down_copy.wait()
        first = pl.ds(pl.multiple_of(a * width, 128), width)
        mine = hid.at[span(s), :]

        acc[base:base + rows, :] = jnp.dot(mine[...], wd[first, :], preferred_element_type=f32)

    def project_other(s):
        rows, base = plan[s], base_of(s)
        second = pl.ds(pl.multiple_of((1 - a) * width, 128), width)
        theirs = hid_in.at[span(s), :]
        hid_copy(s).wait_recv()
        for near, side in enumerate((1 - zb, zb)):
            cols = pl.ds(pl.multiple_of(side * part, 128), part)
            total = acc[base:base + rows, cols] + jnp.dot(
                theirs[...], wd[second, cols], preferred_element_type=f32
            )
            for b in range(XS // 2):
                blocks[side * (XS // 2) + b, 0:rows] = total[:, b * dwidth:(b + 1) * dwidth]
            for kind in (2 * near, 2 * near + 1):
                dsib_out[kind, span(s)] = blocks[block_of(kind, 1 - c), 0:rows].astype(bf16)
            dsib_copy(s, near).start()

    def project(s):
        project_own(s)
        project_other(s)

    def spread(s):
        for kind in (DIAG, ZN, YN, OWN):
            if kind in (DIAG, YN):
                dsib_copy(s, kind // 2).wait_recv()
            total = blocks[block_of(kind, c), 0:plan[s]] + dsib_in[kind, span(s)].astype(f32)
            if kind == OWN:
                keep_d[span(s)] = total
            elif kind == ZN and s < RELAYED:
                keep_n[span(s)] = total
            else:
                dout[kind, span(s)] = total.astype(bf16)

    def send_out(s):
        for kind in (DIAG, YN) if s < RELAYED else (DIAG, YN, ZN):
            dout_copy(s, kind).start()

    def relay_out(s):
        dout_copy(s, DIAG).wait_recv()
        total = keep_n[span(s)] + din[DIAG, span(s)].astype(f32)
        dout[ZN, span(s)] = total.astype(bf16)
        dout_copy(s, ZN).start()

    def relay_outs(s):
        if s < RELAYED:
            relay_out(s)

    def collect(s):
        total = keep_d[span(s)]
        for kind in (YN, ZN) if s < RELAYED else (YN, ZN, DIAG):
            dout_copy(s, kind).wait_recv()
            total = total + din[kind, span(s)].astype(f32)
        keep_d[span(s)] = total

    tok_copy(0).start()
    join(0)
    sibling(0, DIAG)
    sibling(0, ZN)
    own(0, DIAG)
    sibling(0, YN)
    own(0, ZN)
    sibling(0, OWN)
    own(0, YN)
    for s in range(chunks):
        if s > 0:
            for kind in range(3):
                own(s, kind)
        if s < last:
            join(s + 1)
            for kind in range(4):
                sibling(s + 1, kind)
        if s >= 3:
            project(s - 3)
        if s > 0:
            finish(s - 1)
        if s >= 3:
            spread(s - 3)
        relay(s)
    for s in range(last - 2):
        send_out(s)
    project(last - 2)
    project_own(last - 1)
    for s in range(last - 3):
        relay_outs(s)
    finish(last)
    spread(last - 2)
    send_out(last - 2)
    relay_outs(last - 3)
    project_other(last - 1)
    project_own(last)
    relay_outs(last - 2)
    spread(last - 1)
    send_out(last - 1)
    project_other(last)
    spread(last)
    send_out(last)
    out_copies = []
    for s in range(chunks):
        collect(s)
        while 128 * (len(out_copies) + 1) <= starts[s] + plan[s]:
            index = len(out_copies)
            block = pl.ds(128 * index, 128)
            done[:, block] = keep_d[block, :].T.astype(bf16)
            out_copies.append(pltpu.make_async_copy(done.at[:, block], out_t.at[:, block], out_sem.at[index]))
            out_copies[index].start()
    for buffer, sem, target in (
        (tok, tok_s, to_a), (hid, hid_s, to_a), (dsib_out, dsib_s, to_c), (dout, dout_s, to_y)
    ):
        remote(buffer, buffer, sem, raw_sem, target).wait_send()
    sib_copy(last, 0).wait_send()
    for s in range(max(chunks - 2, 0), chunks):
        for piece in range(2):
            if halves[s]:
                z1_copy(s, piece).wait_send()
            y1_copy(s, piece).wait_send()
        z2_copy(s).wait_send()
        if halves[s]:
            y2_copy(s).wait_send()
    for copy in out_copies:
        copy.wait()


def plan_of(count):
    unit = count // sum(PLAN)
    plan = [unit * parts for parts in PLAN]
    halves = [unit * parts for parts in Z_ROWS]
    return plan, halves


def fused(tokens, gate_weight, up_weight, down_weight):
    count, feat = tokens.shape
    depth, half = gate_weight.shape[1:]
    deep, full = down_weight.shape[1:]
    width, dwidth = half // XS, full // XS
    plan, halves = plan_of(count)
    others = [rows - z for rows, z in zip(plan, halves)]
    rows, h0, h1 = max(plan), max(halves), max(others)
    all0, all1 = sum(halves), sum(others)
    bf16, f32 = jnp.bfloat16, jnp.float32
    v = pltpu.VMEM
    buffers = [
        v((feat, count), bf16),
        v((count, feat), bf16),
        v((count, feat), bf16),
        v((count, 2 * feat), bf16),
        v((2, XS, depth, width), bf16),
        v((deep, full), bf16),
        v((4, 2, rows, width), bf16),
        v((4, 2, count, width), bf16),
        v((2, 2, 2, h0, width), bf16),
        v((2, 2, 2, h1, width), bf16),
        v((2, 2, h1, width), bf16),
        v((2, 2, h0, width), bf16),
        v((2, 2, all0, width), bf16),
        v((2, 2, all1, width), bf16),
        v((2, all1, width), bf16),
        v((2, all0, width), bf16),
        v((2, 2, h1, width), f32),
        v((2, 2, h0, width), f32),
        v((2, rows, width), f32),
        v((count, width), bf16),
        v((count, width), bf16),
        v((max(rows, plan[-2] + plan[-1]), full), f32),
        v((XS, rows, dwidth), f32),
        v((count, dwidth), f32),
        v((count, dwidth), f32),
        v((4, count, dwidth), bf16),
        v((4, count, dwidth), bf16),
        v((3, count, dwidth), bf16),
        v((3, count, dwidth), bf16),
        v((dwidth, count), bf16),
    ]
    sem = pltpu.SemaphoreType.DMA
    s = len(plan)
    shapes = [None, None, (s,), (XS,), None, (5,), (s + 3,), (2, 2), (s, 2), (2, 2), (s, 2)]
    shapes += [(2,), (s,), (2,), (s,), None, (s,), None, (s, 2), None, (s, 3), (count // 128,)]
    sems = [sem if shape is None else sem(shape) for shape in shapes]
    hbm = pl.BlockSpec(memory_space=pl.ANY)
    result = pl.pallas_call(
        functools.partial(kernel, plan, halves),
        out_shape=jax.ShapeDtypeStruct((dwidth, count), bf16),
        in_specs=[hbm, hbm, hbm, hbm],
        out_specs=hbm,
        scratch_shapes=buffers + sems,
        compiler_params=pltpu.CompilerParams(
            collective_id=0, has_side_effects=True, vmem_limit_bytes=VMEM_BYTES
        ),
    )(tokens.T, gate_weight, up_weight, down_weight)
    return result.T


def shards(tokens, gate_weight, up_weight, down_weight):
    width = gate_weight.shape[2] // XS
    suits = (
        lax.axis_size("gx") == 2 * XS
        and width % 128 == 0
        and down_weight.shape[2] % 256 == 0
        and tokens.shape[0] % (16 * sum(PLAN)) == 0
        and tokens.shape[0] % 128 == 0
        and tokens.shape[1] % 16 == 0
        and tokens.shape[1] == down_weight.shape[2] // XS
    )
    if suits:
        return fused(tokens, gate_weight, up_weight, down_weight)
    return plain_shards(tokens, gate_weight, up_weight, down_weight)


def solution(mesh):
    placed = (P("groups", "gx"), P("gx", None, None), P("gx", None, None), P("gx", None, None))
    return jax.shard_map(
        shards, mesh=mesh, in_specs=placed, out_specs=P("groups", "gx"), check_vma=False
    )
```
